32 devices in a mesh: outer: 8 (over z, x), inner: 4 (over y, core).
Axes of the slice: x: 2, y: 2, z: 4, core: 2. Of those that a mesh axis runs over, the one named last changes fastest.
Arguments:
- queries: bfloat16 [1024, 2, 4096], P('outer', None, 'inner'), may hold values from -52 to 52
- keys: bfloat16 [1024, 2, 4096], P('outer', None, 'inner'), may hold values from -6 to 6
- values: bfloat16 [1024, 2, 4096], P('outer', None, 'inner'), may hold values from -6 to 6
Outputs:
- attended: bfloat16 [1024, 2, 4096], P(('outer', 'inner'))
The draws below stay inside these ranges and needn't reach their ends.
All inputs are finite; a program needn't handle non-finite values.
Results may differ from the reference program's by a relative error of at most 0.004.
Values may be sent and summed in bfloat16 or wider, within the bound.
A program may use at most 128 MiB of HBM per device.

```python
import math
import jax
import jax.numpy as jnp
from jax import lax

NETWORKS = 2
HEADS = 32
HEAD_DIM = 128
WIDTH = 4096
SEQ = 1024


def key_field(key):
    base = jax.random.fold_in(key, 11)
    field = jnp.clip(jax.random.normal(base, (SEQ, NETWORKS, WIDTH), jnp.float32), -6.0, 6.0)
    return field


def draw_keys(key, part):
    return key_field(key).astype(jnp.bfloat16)


def draw_queries(key, part):
    base = jax.random.fold_in(key, 12)
    result = 3.0 * jnp.clip(jax.random.normal(base, (SEQ, NETWORKS, WIDTH), jnp.float32), -6.0, 6.0)
    return result.astype(jnp.bfloat16)


def steps_of(rng, shape, shards, low, high):
    factor_of, own = 1.0, jax.random.fold_in(rng, 6)
    for axis_at, shards_of in shards:
        draws = jnp.exp(jax.random.uniform(jax.random.fold_in(own, axis_at), (shards_of,), jnp.float32, low / len(shards), high / len(shards)))
        factor_of = factor_of * jnp.repeat(draws, shape[axis_at] // shards_of).reshape([-1 if axis == axis_at else 1 for axis in range(len(shape))])
    return factor_of


def scatter_about(rng, extent, scale, reach, pieces=(), kind=jnp.bfloat16):
    gain = steps_of(rng, extent, pieces, -0.22, 0.18) if pieces else 1.0
    values = jax.random.normal(rng, extent, jnp.float32) * scale * gain
    return jnp.minimum(jnp.maximum(values, -reach), reach).astype(kind)


def setup_inputs(seed: int = 0) -> dict:
    splits = jax.random.split(jax.random.key(seed), 4)
    queries = draw_queries(jax.random.fold_in(splits[3], 71), 0)
    keys = draw_keys(jax.random.fold_in(splits[3], 71), 0)
    values = scatter_about(splits[2], (SEQ, NETWORKS, WIDTH), 1.0, 6.0, ((0, 8), (2, 4)))
    return dict(queries=queries, keys=keys, values=values)


def attend_rows(query_rows, key_rows, value_rows):
    scores = jnp.dot(query_rows, key_rows.T, preferred_element_type=jnp.float32) * (1.0 / math.sqrt(HEAD_DIM))
    peak_rows = lax.optimization_barrier(jnp.max(scores, axis=1, keepdims=True))
    weights = jnp.exp(scores - peak_rows)
    totals = lax.optimization_barrier(jnp.sum(weights, axis=1, keepdims=True))
    numerator = jnp.dot(weights.astype(jnp.bfloat16), value_rows, preferred_element_type=jnp.float32)
    return numerator / totals

def attend_pair(inputs):
    query_rows, key_rows, value_rows = inputs
    blocks = query_rows.reshape(16, SEQ // 16, HEAD_DIM)
    result = lax.map(lambda block: attend_rows(block, key_rows, value_rows), blocks)
    return result.reshape(SEQ, HEAD_DIM)

def split_heads(array):
    return array.reshape(SEQ, NETWORKS, HEADS, HEAD_DIM).transpose(1, 2, 0, 3).reshape(NETWORKS * HEADS, SEQ, HEAD_DIM)

def reference(queries, keys, values):
    averaged = lax.map(attend_pair, (split_heads(queries), split_heads(keys), split_heads(values)))
    averaged = averaged.reshape(NETWORKS, HEADS, SEQ, HEAD_DIM).transpose(2, 0, 1, 3)
    return averaged.reshape(SEQ, NETWORKS, WIDTH).astype(jnp.bfloat16)
```

```python
from functools import partial
import math

import jax
import jax.numpy as jnp
from jax import lax
from jax.experimental import pallas as pl
from jax.experimental.pallas import tpu as pltpu
from jax.sharding import PartitionSpec as P

HEAD_DIM = 128
MESH = pl.DeviceIdType.MESH


def attend_keys(running, key_block, value_block, query_heads, head_count):
    peak_rows, totals, numerator = running
    key_count = key_block.shape[0]
    key_heads = key_block.reshape(key_count, head_count, HEAD_DIM)
    value_heads = value_block.reshape(key_count, head_count, HEAD_DIM)
    scores = jnp.einsum(
        "qhd,khd->qhk", query_heads, key_heads, preferred_element_type=jnp.float32
    ) * (1.0 / math.sqrt(HEAD_DIM))
    new_peaks = jnp.maximum(peak_rows, jnp.max(scores, axis=2))
    shrink = jnp.exp(peak_rows - new_peaks)
    weights = jnp.exp(scores - new_peaks[..., None])
    totals = totals * shrink + jnp.sum(weights, axis=2)
    numerator = numerator * shrink[..., None] + jnp.einsum(
        "qhk,khd->qhd",
        weights.astype(jnp.bfloat16),
        value_heads,
        preferred_element_type=jnp.float32,
    )
    return (new_peaks, totals, numerator)


def attend_piece(running, pieces, query_part, head_count):
    key_rows, value_rows = pieces
    row_count = query_part.shape[0]
    query_heads = query_part.reshape(row_count, head_count, HEAD_DIM)
    block_count = key_rows.shape[0] // row_count
    key_blocks = key_rows.reshape(block_count, row_count, key_rows.shape[1])
    value_blocks = value_rows.reshape(block_count, row_count, value_rows.shape[1])

    def one_block(state, blocks):
        return (attend_keys(state, blocks[0], blocks[1], query_heads, head_count), None)

    running, unused = lax.scan(one_block, running, (key_blocks, value_blocks))
    return running


def start_state(row_count, head_count):
    peak_rows = jnp.full((row_count, head_count), -jnp.inf, jnp.float32)
    totals = jnp.zeros((row_count, head_count), jnp.float32)
    numerator = jnp.zeros((row_count, head_count, HEAD_DIM), jnp.float32)
    return (peak_rows, totals, numerator)


def finish_state(running):
    peak_rows, totals, numerator = running
    averaged = numerator / totals[..., None]
    return averaged.reshape(numerator.shape[0], -1).astype(jnp.bfloat16)


def flatten(array):
    return array.reshape(array.shape[0], array.shape[1] * array.shape[2])


def per_device_split(queries, keys, values):
    tok_rows, networks, local_cols = queries.shape
    full_q, full_k, full_v = (
        lax.all_to_all(array, "inner", split_axis=0, concat_axis=2, tiled=True)
        for array in (queries, keys, values)
    )
    unit_rows = full_q.shape[0]
    full_cols = full_q.shape[2]
    query_part, key_part, value_part = (
        lax.all_to_all(flatten(array), "outer", split_axis=1, concat_axis=0, tiled=True)
        for array in (full_q, full_k, full_v)
    )
    head_count = query_part.shape[1] // HEAD_DIM
    running = attend_piece(
        start_state(query_part.shape[0], head_count),
        (
            lax.all_gather(key_part, "inner", axis=0, tiled=True),
            lax.all_gather(value_part, "inner", axis=0, tiled=True),
        ),
        query_part,
        head_count,
    )
    gathered = lax.all_to_all(
        finish_state(running), "outer", split_axis=0, concat_axis=1, tiled=True
    )
    return gathered.reshape(unit_rows, networks, full_cols)


def attend_block(query, key, value):
    raw = lax.dot_general(
        query, key, (((1,), (1,)), ((), ())), preferred_element_type=jnp.float32
    )
    peak = jnp.max(raw, axis=1, keepdims=True)
    weights = jnp.exp2((raw - peak) * (math.log2(math.e) / math.sqrt(HEAD_DIM)))
    totals = jnp.sum(weights, axis=1, keepdims=True)
    numerator = jnp.dot(
        weights.astype(jnp.bfloat16), value, preferred_element_type=jnp.float32
    )
    return (numerator / totals).astype(jnp.bfloat16)


def exchange_kernel(
    outer, inner, networks, local_heads, per,
    q_ref, k_ref, v_ref, out_ref,
    q_buf, k_buf, v_buf, o_buf,
    local_sem, in_send, in_recv, out_send, out_recv,
):
    me_o, me_i = lax.axis_index("outer"), lax.axis_index("inner")
    tokens = q_ref.shape[1]
    out_rows = out_ref.shape[1]
    all_heads = local_heads * inner
    half = outer // 2
    my_half, my_rest = me_o // half, me_o % half
    refs, bufs = (k_ref, v_ref, q_ref), (k_buf, v_buf, q_buf)

    def partner(step, sign):
        side = jnp.where(step < half, 1 - my_half, my_half)
        return side * half + (my_rest + sign * step + 2 * outer) % half

    def rows_of(block):
        return pl.ds(pl.multiple_of(block * tokens, tokens), tokens)

    steps = [step for step in range(outer) if step != half]

    def in_copy(unit, which, step, sign):
        other = partner(step, sign)
        target = other if sign == 1 else me_o
        source = me_o if sign == 1 else other
        return pltpu.make_async_remote_copy(
            src_ref=refs[which].at[target * per + unit],
            dst_ref=bufs[which].at[unit, rows_of(source)],
            send_sem=in_send.at[unit * 3 + which, step],
            recv_sem=in_recv.at[unit * 3 + which, step],
            device_id=(other, me_i),
            device_id_type=MESH,
        )

    def own_copy(unit, which):
        return pltpu.make_async_copy(
            refs[which].at[me_o * per + unit],
            bufs[which].at[unit, rows_of(me_o)],
            local_sem.at[unit * 3 + which],
        )

    def slot_of(source_o, source_i, unit):
        pair = source_o * per + unit
        return (pair // local_heads) * all_heads + source_i * local_heads + pair % local_heads

    def out_copy(unit, block, part):
        return pltpu.make_async_remote_copy(
            src_ref=o_buf.at[unit, pl.ds(pl.multiple_of(block * tokens + part * out_rows, out_rows), out_rows)],
            dst_ref=out_ref.at[slot_of(me_o, me_i, unit)],
            send_sem=out_send.at[unit, block * inner + part],
            recv_sem=out_recv.at[slot_of(me_o, me_i, unit)],
            device_id=(block, part),
            device_id_type=MESH,
        )

    def out_own(unit):
        return pltpu.make_async_copy(
            o_buf.at[unit, pl.ds(pl.multiple_of(me_o * tokens + me_i * out_rows, out_rows), out_rows)],
            out_ref.at[slot_of(me_o, me_i, unit)],
            out_recv.at[slot_of(me_o, me_i, unit)],
        )

    barrier = pltpu.get_barrier_semaphore()

    def greet(index, carry):
        other = (me_o * inner + me_i + index) % (outer * inner)
        pl.semaphore_signal(
            barrier, inc=1, device_id=(other // inner, other % inner), device_id_type=MESH
        )
        return carry

    lax.fori_loop(1, outer * inner, greet, 0)
    for unit in range(per):
        for which in range(3):
            own_copy(unit, which).start()
    pl.semaphore_wait(barrier, outer * inner - 1)

    for unit in range(per):
        for which in range(3):
            for step in steps:
                in_copy(unit, which, step, 1).start()

    def compute(unit, block):
        o_buf[unit, rows_of(block)] = attend_block(
            q_buf[unit, rows_of(block)], k_buf[unit], v_buf[unit]
        )

    for unit in range(per):
        for which in range(3):
            own_copy(unit, which).wait()
        for which in range(2):
            for step in steps:
                in_copy(unit, which, step, -1).wait_recv()

        def one_block(index, carry):
            step = jnp.where(index < half, index, index + 1)
            in_copy(unit, 2, step, -1).wait_recv()
            block = partner(step, -1)
            compute(unit, block)
            for part in range(inner):
                out_copy(unit, block, part).start()
            return carry

        lax.fori_loop(0, outer - 1, one_block, 0)
        compute(unit, me_o)
        for shift in range(1, inner):
            out_copy(unit, me_o, (me_i + shift) % inner).start()
        out_own(unit).start()

    for unit in range(per):
        for which in range(3):
            for step in steps:
                in_copy(unit, which, step, 1).wait_send()

        def sent(index, carry):
            other = (me_o * inner + me_i + index) % (outer * inner)
            out_copy(unit, other // inner, other % inner).wait_send()
            return carry

        lax.fori_loop(1, outer * inner, sent, 0)

        def received(index, carry):
            other = (me_o * inner + me_i + index) % (outer * inner)
            slot = slot_of(other // inner, other % inner, unit)
            pltpu.make_async_remote_copy(
                src_ref=o_buf.at[unit, pl.ds(0, out_rows)],
                dst_ref=out_ref.at[slot],
                send_sem=out_send.at[unit, 0],
                recv_sem=out_recv.at[slot],
                device_id=(other // inner, other % inner),
                device_id_type=MESH,
            ).wait_recv()
            return carry

        lax.fori_loop(1, outer * inner, received, 0)
        out_own(unit).wait()


def per_device(outer, inner, queries, keys, values):
    tokens, networks, local_cols = queries.shape
    local_heads = local_cols // HEAD_DIM
    pairs = networks * local_heads
    per = pairs // outer
    seq = tokens * outer
    out_rows = tokens // inner
    slots = pairs * inner

    def by_pair(array):
        split = array.reshape(tokens, networks, local_heads, HEAD_DIM)
        return split.transpose(1, 2, 0, 3).reshape(pairs, tokens, HEAD_DIM)

    buffer = pltpu.VMEM((per, seq, HEAD_DIM), jnp.bfloat16)
    gathered = pl.pallas_call(
        partial(exchange_kernel, outer, inner, networks, local_heads, per),
        out_shape=jax.ShapeDtypeStruct((slots, out_rows, HEAD_DIM), jnp.bfloat16),
        in_specs=[pl.BlockSpec(memory_space=pl.ANY)] * 3,
        out_specs=pl.BlockSpec(memory_space=pl.ANY),
        scratch_shapes=[
            buffer, buffer, buffer, buffer,
            pltpu.SemaphoreType.DMA((per * 3,)),
            pltpu.SemaphoreType.DMA((per * 3, outer)),
            pltpu.SemaphoreType.DMA((per * 3, outer)),
            pltpu.SemaphoreType.DMA((per, outer * inner)),
            pltpu.SemaphoreType.DMA((slots,)),
        ],
        compiler_params=pltpu.CompilerParams(collective_id=0, has_side_effects=True),
    )(by_pair(queries), by_pair(keys), by_pair(values))
    joined = gathered.reshape(networks, local_heads * inner, out_rows, HEAD_DIM)
    return joined.transpose(2, 0, 1, 3).reshape(out_rows, networks, local_cols * inner)


def solution(mesh):
    outer, inner = mesh.shape["outer"], mesh.shape["inner"]

    def body(queries, keys, values):
        pairs = queries.shape[1] * queries.shape[2] // HEAD_DIM
        if outer % 2 == 0 and pairs % outer == 0:
            return per_device(outer, inner, queries, keys, values)
        return per_device_split(queries, keys, values)

    return jax.shard_map(
        body,
        mesh=mesh,
        in_specs=(P("outer", None, "inner"),) * 3,
        out_specs=P(("outer", "inner"), None, None),
        check_vma=False,
    )
```

```python
from functools import partial
import math

import jax
import jax.numpy as jnp
from jax import lax
from jax.experimental import pallas as pl
from jax.experimental.pallas import tpu as pltpu
from jax.sharding import PartitionSpec as P

HEAD_DIM = 128
MESH = pl.DeviceIdType.MESH


def attend_keys(running, key_block, value_block, query_heads, head_count):
    peak_rows, totals, numerator = running
    key_count = key_block.shape[0]
    key_heads = key_block.reshape(key_count, head_count, HEAD_DIM)
    value_heads = value_block.reshape(key_count, head_count, HEAD_DIM)
    scores = jnp.einsum(
        "qhd,khd->qhk", query_heads, key_heads, preferred_element_type=jnp.float32
    ) * (1.0 / math.sqrt(HEAD_DIM))
    new_peaks = jnp.maximum(peak_rows, jnp.max(scores, axis=2))
    shrink = jnp.exp(peak_rows - new_peaks)
    weights = jnp.exp(scores - new_peaks[..., None])
    totals = totals * shrink + jnp.sum(weights, axis=2)
    numerator = numerator * shrink[..., None] + jnp.einsum(
        "qhk,khd->qhd",
        weights.astype(jnp.bfloat16),
        value_heads,
        preferred_element_type=jnp.float32,
    )
    return (new_peaks, totals, numerator)


def attend_piece(running, pieces, query_part, head_count):
    key_rows, value_rows = pieces
    row_count = query_part.shape[0]
    query_heads = query_part.reshape(row_count, head_count, HEAD_DIM)
    block_count = key_rows.shape[0] // row_count
    key_blocks = key_rows.reshape(block_count, row_count, key_rows.shape[1])
    value_blocks = value_rows.reshape(block_count, row_count, value_rows.shape[1])

    def one_block(state, blocks):
        return (attend_keys(state, blocks[0], blocks[1], query_heads, head_count), None)

    running, unused = lax.scan(one_block, running, (key_blocks, value_blocks))
    return running


def start_state(row_count, head_count):
    peak_rows = jnp.full((row_count, head_count), -jnp.inf, jnp.float32)
    totals = jnp.zeros((row_count, head_count), jnp.float32)
    numerator = jnp.zeros((row_count, head_count, HEAD_DIM), jnp.float32)
    return (peak_rows, totals, numerator)


def finish_state(running):
    peak_rows, totals, numerator = running
    averaged = numerator / totals[..., None]
    return averaged.reshape(numerator.shape[0], -1).astype(jnp.bfloat16)


def flatten(array):
    return array.reshape(array.shape[0], array.shape[1] * array.shape[2])


def per_device_split(queries, keys, values):
    tok_rows, networks, local_cols = queries.shape
    full_q, full_k, full_v = (
        lax.all_to_all(array, "inner", split_axis=0, concat_axis=2, tiled=True)
        for array in (queries, keys, values)
    )
    unit_rows = full_q.shape[0]
    full_cols = full_q.shape[2]
    query_part, key_part, value_part = (
        lax.all_to_all(flatten(array), "outer", split_axis=1, concat_axis=0, tiled=True)
        for array in (full_q, full_k, full_v)
    )
    head_count = query_part.shape[1] // HEAD_DIM
    running = attend_piece(
        start_state(query_part.shape[0], head_count),
        (
            lax.all_gather(key_part, "inner", axis=0, tiled=True),
            lax.all_gather(value_part, "inner", axis=0, tiled=True),
        ),
        query_part,
        head_count,
    )
    gathered = lax.all_to_all(
        finish_state(running), "outer", split_axis=0, concat_axis=1, tiled=True
    )
    return gathered.reshape(unit_rows, networks, full_cols)


def attend_block(query, key, value):
    raw = lax.dot_general(
        query, key, (((1,), (1,)), ((), ())), preferred_element_type=jnp.float32
    )
    peak = jnp.max(raw, axis=1, keepdims=True)
    weights = jnp.exp2((raw - peak) * (math.log2(math.e) / math.sqrt(HEAD_DIM)))
    totals = jnp.sum(weights, axis=1, keepdims=True)
    numerator = jnp.dot(
        weights.astype(jnp.bfloat16), value, preferred_element_type=jnp.float32
    )
    return (numerator / totals).astype(jnp.bfloat16)


def exchange_kernel(
    outer, inner, heads,
    q_ref, k_ref, v_ref, out_ref,
    q_raw, k_raw, v_raw, k_buf, v_buf, o_raw,
    local_sem, in_send, in_recv, out_send, out_recv,
):
    me_o, me_i = lax.axis_index("outer"), lax.axis_index("inner")
    tokens, networks, local_cols = q_ref.shape
    out_rows = out_ref.shape[0]
    half = outer // 2
    my_half, my_rest = me_o // half, me_o % half
    refs, raws = (k_ref, v_ref, q_ref), (k_raw, v_raw, q_raw)

    def partner(step, sign):
        side = jnp.where(step < half, 1 - my_half, my_half)
        return side * half + (my_rest + sign * step + 2 * outer) % half

    def rows_of(block):
        return pl.ds(pl.multiple_of(block * tokens, tokens), tokens)

    def cols_of(head):
        return pl.ds(pl.multiple_of(head * HEAD_DIM, HEAD_DIM), HEAD_DIM)

    steps = [step for step in range(outer) if step != half]

    def in_copy(head, which, step, sign):
        other = partner(step, sign)
        target = other if sign == 1 else me_o
        source = me_o if sign == 1 else other
        return pltpu.make_async_remote_copy(
            src_ref=refs[which].at[:, :, cols_of(target * heads + head)],
            dst_ref=raws[which].at[head, rows_of(source)],
            send_sem=in_send.at[head * 3 + which, step],
            recv_sem=in_recv.at[head * 3 + which, step],
            device_id=(other, me_i),
            device_id_type=MESH,
        )

    def own_copy(head, which):
        return pltpu.make_async_copy(
            refs[which].at[:, :, cols_of(me_o * heads + head)],
            raws[which].at[head, rows_of(me_o)],
            local_sem.at[head * 3 + which],
        )

    def out_cols(source_o, source_i, head):
        return cols_of(source_i * (local_cols // HEAD_DIM) + source_o * heads + head)

    def out_slice(block, part):
        return pl.ds(block * tokens + part * out_rows, out_rows)

    def out_copy(head, block, part):
        return pltpu.make_async_remote_copy(
            src_ref=o_raw.at[head, out_slice(block, part)],
            dst_ref=out_ref.at[:, :, out_cols(me_o, me_i, head)],
            send_sem=out_send.at[head, block * inner + part],
            recv_sem=out_recv.at[head, me_o * inner + me_i],
            device_id=(block, part),
            device_id_type=MESH,
        )

    def out_own(head):
        return pltpu.make_async_copy(
            o_raw.at[head, out_slice(me_o, me_i)],
            out_ref.at[:, :, out_cols(me_o, me_i, head)],
            out_recv.at[head, me_o * inner + me_i],
        )

    barrier = pltpu.get_barrier_semaphore()

    def greet(index, carry):
        other = (me_o * inner + me_i + index) % (outer * inner)
        pl.semaphore_signal(
            barrier, inc=1, device_id=(other // inner, other % inner), device_id_type=MESH
        )
        return carry

    lax.fori_loop(1, outer * inner, greet, 0)
    for head in range(heads):
        for which in range(3):
            own_copy(head, which).start()
    pl.semaphore_wait(barrier, outer * inner - 1)

    for head in range(heads):
        for which in range(3):
            for step in steps:
                in_copy(head, which, step, 1).start()

    both = networks * tokens
    split_row = lax.broadcasted_iota(jnp.int32, (both, both), 0)
    split_col = lax.broadcasted_iota(jnp.int32, (both, both), 1)
    split = (split_col == (split_row % tokens) * networks + split_row // tokens)
    split = split.astype(jnp.float32).astype(jnp.bfloat16)
    join = (split_row == (split_col % tokens) * networks + split_col // tokens)
    join = join.astype(jnp.float32).astype(jnp.bfloat16)

    def separate(raw, head, block):
        mixed = raw[head, rows_of(block)].reshape(both, HEAD_DIM)
        return jnp.dot(split, mixed, preferred_element_type=jnp.float32).astype(jnp.bfloat16)

    def place(head, which, block):
        apart = separate(raws[which], head, block)
        kept = (k_buf, v_buf)[which]
        for network in range(networks):
            kept[network, rows_of(block)] = apart[network * tokens:(network + 1) * tokens]

    def compute(head, block):
        query = separate(q_raw, head, block)
        parts = [
            attend_block(query[n * tokens:(n + 1) * tokens], k_buf[n], v_buf[n])
            for n in range(networks)
        ]
        mixed = jnp.dot(join, jnp.concatenate(parts, axis=0), preferred_element_type=jnp.float32)
        o_raw[head, rows_of(block)] = mixed.astype(jnp.bfloat16).reshape(
            tokens, networks, HEAD_DIM
        )

    for head in range(heads):
        for which in range(3):
            own_copy(head, which).wait()
        for which in range(2):
            place(head, which, me_o)

            def one_place(index, carry):
                step = jnp.where(index < half, index, index + 1)
                in_copy(head, which, step, -1).wait_recv()
                place(head, which, partner(step, -1))
                return carry

            lax.fori_loop(0, outer - 1, one_place, 0)

        def one_block(index, carry):
            step = jnp.where(index < half, index, index + 1)
            in_copy(head, 2, step, -1).wait_recv()
            block = partner(step, -1)
            compute(head, block)
            for part in range(inner):
                out_copy(head, block, part).start()
            return carry

        lax.fori_loop(0, outer - 1, one_block, 0)
        compute(head, me_o)
        for shift in range(1, inner):
            out_copy(head, me_o, (me_i + shift) % inner).start()
        out_own(head).start()

    for head in range(heads):
        for which in range(3):
            for step in steps:
                in_copy(head, which, step, 1).wait_send()

        def sent(index, carry):
            other = (me_o * inner + me_i + index) % (outer * inner)
            out_copy(head, other // inner, other % inner).wait_send()
            return carry

        lax.fori_loop(1, outer * inner, sent, 0)

        def received(index, carry):
            other = (me_o * inner + me_i + index) % (outer * inner)
            pltpu.make_async_remote_copy(
                src_ref=o_raw.at[head, pl.ds(0, out_rows)],
                dst_ref=out_ref.at[:, :, out_cols(other // inner, other % inner, head)],
                send_sem=out_send.at[head, 0],
                recv_sem=out_recv.at[head, other],
                device_id=(other // inner, other % inner),
                device_id_type=MESH,
            ).wait_recv()
            return carry

        lax.fori_loop(1, outer * inner, received, 0)
        out_own(head).wait()


def per_device(outer, inner, queries, keys, values):
    tokens, networks, local_cols = queries.shape
    heads = local_cols // HEAD_DIM // outer
    seq = tokens * outer
    out_rows = tokens // inner
    raw = pltpu.VMEM((heads, seq, networks, HEAD_DIM), jnp.bfloat16)
    kept = pltpu.VMEM((networks, seq, HEAD_DIM), jnp.bfloat16)
    return pl.pallas_call(
        partial(exchange_kernel, outer, inner, heads),
        out_shape=jax.ShapeDtypeStruct((out_rows, networks, local_cols * inner), jnp.bfloat16),
        in_specs=[pl.BlockSpec(memory_space=pl.ANY)] * 3,
        out_specs=pl.BlockSpec(memory_space=pl.ANY),
        scratch_shapes=[
            raw, raw, raw, kept, kept, raw,
            pltpu.SemaphoreType.DMA((heads * 3,)),
            pltpu.SemaphoreType.DMA((heads * 3, outer)),
            pltpu.SemaphoreType.DMA((heads * 3, outer)),
            pltpu.SemaphoreType.DMA((heads, outer * inner)),
            pltpu.SemaphoreType.DMA((heads, outer * inner)),
        ],
        compiler_params=pltpu.CompilerParams(collective_id=0, has_side_effects=True),
    )(queries, keys, values)


def solution(mesh):
    outer, inner = mesh.shape["outer"], mesh.shape["inner"]

    def body(queries, keys, values):
        heads = queries.shape[2] // HEAD_DIM
        if outer % 2 == 0 and heads % outer == 0:
            return per_device(outer, inner, queries, keys, values)
        return per_device_split(queries, keys, values)

    return jax.shard_map(
        body,
        mesh=mesh,
        in_specs=(P("outer", None, "inner"),) * 3,
        out_specs=P(("outer", "inner"), None, None),
        check_vma=False,
    )
```

```python
from functools import partial
import math

import jax
import jax.numpy as jnp
from jax import lax
from jax.experimental import pallas as pl
from jax.experimental.pallas import tpu as pltpu
from jax.sharding import PartitionSpec as P

HEAD_DIM = 128
MESH = pl.DeviceIdType.MESH


def attend_keys(running, key_block, value_block, query_heads, head_count):
    peak_rows, totals, numerator = running
    key_count = key_block.shape[0]
    key_heads = key_block.reshape(key_count, head_count, HEAD_DIM)
    value_heads = value_block.reshape(key_count, head_count, HEAD_DIM)
    scores = jnp.einsum(
        "qhd,khd->qhk", query_heads, key_heads, preferred_element_type=jnp.float32
    ) * (1.0 / math.sqrt(HEAD_DIM))
    new_peaks = jnp.maximum(peak_rows, jnp.max(scores, axis=2))
    shrink = jnp.exp(peak_rows - new_peaks)
    weights = jnp.exp(scores - new_peaks[..., None])
    totals = totals * shrink + jnp.sum(weights, axis=2)
    numerator = numerator * shrink[..., None] + jnp.einsum(
        "qhk,khd->qhd",
        weights.astype(jnp.bfloat16),
        value_heads,
        preferred_element_type=jnp.float32,
    )
    return (new_peaks, totals, numerator)


def attend_piece(running, pieces, query_part, head_count):
    key_rows, value_rows = pieces
    row_count = query_part.shape[0]
    query_heads = query_part.reshape(row_count, head_count, HEAD_DIM)
    block_count = key_rows.shape[0] // row_count
    key_blocks = key_rows.reshape(block_count, row_count, key_rows.shape[1])
    value_blocks = value_rows.reshape(block_count, row_count, value_rows.shape[1])

    def one_block(state, blocks):
        return (attend_keys(state, blocks[0], blocks[1], query_heads, head_count), None)

    running, unused = lax.scan(one_block, running, (key_blocks, value_blocks))
    return running


def start_state(row_count, head_count):
    peak_rows = jnp.full((row_count, head_count), -jnp.inf, jnp.float32)
    totals = jnp.zeros((row_count, head_count), jnp.float32)
    numerator = jnp.zeros((row_count, head_count, HEAD_DIM), jnp.float32)
    return (peak_rows, totals, numerator)


def finish_state(running):
    peak_rows, totals, numerator = running
    averaged = numerator / totals[..., None]
    return averaged.reshape(numerator.shape[0], -1).astype(jnp.bfloat16)


def flatten(array):
    return array.reshape(array.shape[0], array.shape[1] * array.shape[2])


def per_device_split(queries, keys, values):
    tok_rows, networks, local_cols = queries.shape
    full_q, full_k, full_v = (
        lax.all_to_all(array, "inner", split_axis=0, concat_axis=2, tiled=True)
        for array in (queries, keys, values)
    )
    unit_rows = full_q.shape[0]
    full_cols = full_q.shape[2]
    query_part, key_part, value_part = (
        lax.all_to_all(flatten(array), "outer", split_axis=1, concat_axis=0, tiled=True)
        for array in (full_q, full_k, full_v)
    )
    head_count = query_part.shape[1] // HEAD_DIM
    running = attend_piece(
        start_state(query_part.shape[0], head_count),
        (
            lax.all_gather(key_part, "inner", axis=0, tiled=True),
            lax.all_gather(value_part, "inner", axis=0, tiled=True),
        ),
        query_part,
        head_count,
    )
    gathered = lax.all_to_all(
        finish_state(running), "outer", split_axis=0, concat_axis=1, tiled=True
    )
    return gathered.reshape(unit_rows, networks, full_cols)


def attend_block(query, key, value):
    raw = lax.dot_general(
        query, key, (((1,), (1,)), ((), ())), preferred_element_type=jnp.float32
    )
    peak = jnp.max(raw, axis=1, keepdims=True)
    weights = jnp.exp2((raw - peak) * (math.log2(math.e) / math.sqrt(HEAD_DIM)))
    totals = jnp.sum(weights, axis=1, keepdims=True)
    numerator = jnp.dot(
        weights.astype(jnp.bfloat16), value, preferred_element_type=jnp.float32
    )
    return (numerator / totals).astype(jnp.bfloat16)


def exchange_kernel(
    outer, inner, heads,
    q_ref, k_ref, v_ref, out_ref,
    q_raw, k_raw, v_raw, k_buf, v_buf, o_raw,
    q_src, k_src, v_src, src_sem, local_sem, in_send, in_recv, out_send, out_recv,
):
    me_o, me_i = lax.axis_index("outer"), lax.axis_index("inner")
    tokens, networks, local_cols = q_ref.shape
    out_rows = out_ref.shape[0]
    half = outer // 2
    my_half, my_rest = me_o // half, me_o % half
    refs, raws = (k_src, v_src, q_src), (k_raw, v_raw, q_raw)

    def partner(step, sign):
        side = jnp.where(step < half, 1 - my_half, my_half)
        return side * half + (my_rest + sign * step + 2 * outer) % half

    def rows_of(block):
        return pl.ds(pl.multiple_of(block * tokens, tokens), tokens)

    def cols_of(head):
        return pl.ds(pl.multiple_of(head * HEAD_DIM, HEAD_DIM), HEAD_DIM)

    steps = [step for step in range(outer) if step != half]

    def in_copy(head, which, step, sign):
        other = partner(step, sign)
        target = other if sign == 1 else me_o
        source = me_o if sign == 1 else other
        return pltpu.make_async_remote_copy(
            src_ref=refs[which].at[:, :, cols_of(target * heads + head)],
            dst_ref=raws[which].at[head, rows_of(source)],
            send_sem=in_send,
            recv_sem=in_recv.at[head * 3 + which, step],
            device_id=(other, me_i),
            device_id_type=MESH,
        )

    def own_copy(head, which):
        return pltpu.make_async_copy(
            refs[which].at[:, :, cols_of(me_o * heads + head)],
            raws[which].at[head, rows_of(me_o)],
            local_sem.at[head * 3 + which],
        )

    def out_cols(source_o, source_i, head):
        return cols_of(source_i * (local_cols // HEAD_DIM) + source_o * heads + head)

    def out_slice(block, part):
        return pl.ds(block * tokens + part * out_rows, out_rows)

    def out_copy(head, block, part):
        return pltpu.make_async_remote_copy(
            src_ref=o_raw.at[head, out_slice(block, part)],
            dst_ref=out_ref.at[:, :, out_cols(me_o, me_i, head)],
            send_sem=out_send,
            recv_sem=out_recv,
            device_id=(block, part),
            device_id_type=MESH,
        )

    def out_own(head):
        return pltpu.make_async_copy(
            o_raw.at[head, out_slice(me_o, me_i)],
            out_ref.at[:, :, out_cols(me_o, me_i, head)],
            out_recv,
        )

    barrier = pltpu.get_barrier_semaphore()

    sources = [
        pltpu.make_async_copy(ref, kept, src_sem.at[which])
        for which, (ref, kept) in enumerate(zip((k_ref, v_ref, q_ref), refs))
    ]
    for copy in sources:
        copy.start()
    ends = [partner(step, 1) for step in steps]
    for shift in range(inner):
        part = (me_i + shift) % inner
        for other in ends:
            pl.semaphore_signal(barrier, inc=1, device_id=(other, part), device_id_type=MESH)
        if shift:
            pl.semaphore_signal(barrier, inc=1, device_id=(me_o, part), device_id_type=MESH)
    for copy in sources:
        copy.wait()
    pl.semaphore_wait(barrier, outer * inner - 1)

    for head in range(heads):
        for which in range(3):
            for step in steps:
                in_copy(head, which, step, 1).start()
            own_copy(head, which).start()

    both = networks * tokens
    split_row = lax.broadcasted_iota(jnp.int32, (both, both), 0)
    split_col = lax.broadcasted_iota(jnp.int32, (both, both), 1)
    split = (split_col == (split_row % tokens) * networks + split_row // tokens)
    split = split.astype(jnp.float32).astype(jnp.bfloat16)
    join = (split_row == (split_col % tokens) * networks + split_col // tokens)
    join = join.astype(jnp.float32).astype(jnp.bfloat16)

    def separate(raw, head, block):
        mixed = raw[head, rows_of(block)].reshape(both, HEAD_DIM)
        return jnp.dot(split, mixed, preferred_element_type=jnp.float32).astype(jnp.bfloat16)

    def place(head, which, block):
        apart = separate(raws[which], head, block)
        kept = (k_buf, v_buf)[which]
        for network in range(networks):
            kept[network, rows_of(block)] = apart[network * tokens:(network + 1) * tokens]

    def compute(head, block):
        query = separate(q_raw, head, block)
        parts = [
            attend_block(query[n * tokens:(n + 1) * tokens], k_buf[n], v_buf[n])
            for n in range(networks)
        ]
        mixed = jnp.dot(join, jnp.concatenate(parts, axis=0), preferred_element_type=jnp.float32)
        o_raw[head, rows_of(block)] = mixed.astype(jnp.bfloat16).reshape(
            tokens, networks, HEAD_DIM
        )

    for head in range(heads):
        for which in range(3):
            own_copy(head, which).wait()
        for which in range(2):
            place(head, which, me_o)

            def one_place(index, carry):
                step = jnp.where(index < half, index, index + 1)
                in_copy(head, which, step, -1).wait_recv()
                place(head, which, partner(step, -1))
                return carry

            lax.fori_loop(0, outer - 1, one_place, 0)

        compute(head, me_o)
        for shift in range(1, inner):
            out_copy(head, me_o, (me_i + shift) % inner).start()
        out_own(head).start()

        def one_block(index, carry):
            step = jnp.where(index < half, index, index + 1)
            in_copy(head, 2, step, -1).wait_recv()
            block = partner(step, -1)
            compute(head, block)
            for part in range(inner):
                out_copy(head, block, part).start()
            return carry

        lax.fori_loop(0, outer - 1, one_block, 0)

    def wait_bytes(ref, sem):
        pltpu.make_async_copy(ref, ref, sem).wait()

    for head in range(heads):
        for raw in raws:
            wait_bytes(raw.at[head, pl.ds(0, tokens * (outer - 1))], in_send)
        wait_bytes(o_raw.at[head, pl.ds(0, tokens * outer - out_rows)], out_send)
    wait_bytes(out_ref, out_recv)


def per_device(outer, inner, queries, keys, values):
    tokens, networks, local_cols = queries.shape
    heads = local_cols // HEAD_DIM // outer
    seq = tokens * outer
    out_rows = tokens // inner
    raw = pltpu.VMEM((heads, seq, networks, HEAD_DIM), jnp.bfloat16)
    kept = pltpu.VMEM((networks, seq, HEAD_DIM), jnp.bfloat16)
    return pl.pallas_call(
        partial(exchange_kernel, outer, inner, heads),
        out_shape=jax.ShapeDtypeStruct((out_rows, networks, local_cols * inner), jnp.bfloat16),
        in_specs=[pl.BlockSpec(memory_space=pl.ANY)] * 3,
        out_specs=pl.BlockSpec(memory_space=pl.ANY),
        scratch_shapes=[
            raw, raw, raw, kept, kept, raw,
            *[pltpu.VMEM(queries.shape, jnp.bfloat16)] * 3,
            pltpu.SemaphoreType.DMA((3,)),
            pltpu.SemaphoreType.DMA((heads * 3,)),
            pltpu.SemaphoreType.DMA,
            pltpu.SemaphoreType.DMA((heads * 3, outer)),
            pltpu.SemaphoreType.DMA,
            pltpu.SemaphoreType.DMA,
        ],
        compiler_params=pltpu.CompilerParams(collective_id=0, has_side_effects=True),
    )(queries, keys, values)


def solution(mesh):
    outer, inner = mesh.shape["outer"], mesh.shape["inner"]

    def body(queries, keys, values):
        heads = queries.shape[2] // HEAD_DIM
        if outer % 2 == 0 and heads % outer == 0:
            return per_device(outer, inner, queries, keys, values)
        return per_device_split(queries, keys, values)

    return jax.shard_map(
        body,
        mesh=mesh,
        in_specs=(P("outer", None, "inner"),) * 3,
        out_specs=P(("outer", "inner"), None, None),
        check_vma=False,
    )
```

```python
from functools import partial
import math

import jax
import jax.numpy as jnp
from jax import lax
from jax.experimental import pallas as pl
from jax.experimental.pallas import tpu as pltpu
from jax.sharding import PartitionSpec as P

HEAD_DIM = 128
MESH = pl.DeviceIdType.MESH


def attend_keys(running, key_block, value_block, query_heads, head_count):
    peak_rows, totals, numerator = running
    key_count = key_block.shape[0]
    key_heads = key_block.reshape(key_count, head_count, HEAD_DIM)
    value_heads = value_block.reshape(key_count, head_count, HEAD_DIM)
    scores = jnp.einsum(
        "qhd,khd->qhk", query_heads, key_heads, preferred_element_type=jnp.float32
    ) * (1.0 / math.sqrt(HEAD_DIM))
    new_peaks = jnp.maximum(peak_rows, jnp.max(scores, axis=2))
    shrink = jnp.exp(peak_rows - new_peaks)
    weights = jnp.exp(scores - new_peaks[..., None])
    totals = totals * shrink + jnp.sum(weights, axis=2)
    numerator = numerator * shrink[..., None] + jnp.einsum(
        "qhk,khd->qhd",
        weights.astype(jnp.bfloat16),
        value_heads,
        preferred_element_type=jnp.float32,
    )
    return (new_peaks, totals, numerator)


def attend_piece(running, pieces, query_part, head_count):
    key_rows, value_rows = pieces
    row_count = query_part.shape[0]
    query_heads = query_part.reshape(row_count, head_count, HEAD_DIM)
    block_count = key_rows.shape[0] // row_count
    key_blocks = key_rows.reshape(block_count, row_count, key_rows.shape[1])
    value_blocks = value_rows.reshape(block_count, row_count, value_rows.shape[1])

    def one_block(state, blocks):
        return (attend_keys(state, blocks[0], blocks[1], query_heads, head_count), None)

    running, unused = lax.scan(one_block, running, (key_blocks, value_blocks))
    return running


def start_state(row_count, head_count):
    peak_rows = jnp.full((row_count, head_count), -jnp.inf, jnp.float32)
    totals = jnp.zeros((row_count, head_count), jnp.float32)
    numerator = jnp.zeros((row_count, head_count, HEAD_DIM), jnp.float32)
    return (peak_rows, totals, numerator)


def finish_state(running):
    peak_rows, totals, numerator = running
    averaged = numerator / totals[..., None]
    return averaged.reshape(numerator.shape[0], -1).astype(jnp.bfloat16)


def flatten(array):
    return array.reshape(array.shape[0], array.shape[1] * array.shape[2])


def per_device_split(queries, keys, values):
    tok_rows, networks, local_cols = queries.shape
    full_q, full_k, full_v = (
        lax.all_to_all(array, "inner", split_axis=0, concat_axis=2, tiled=True)
        for array in (queries, keys, values)
    )
    unit_rows = full_q.shape[0]
    full_cols = full_q.shape[2]
    query_part, key_part, value_part = (
        lax.all_to_all(flatten(array), "outer", split_axis=1, concat_axis=0, tiled=True)
        for array in (full_q, full_k, full_v)
    )
    head_count = query_part.shape[1] // HEAD_DIM
    running = attend_piece(
        start_state(query_part.shape[0], head_count),
        (
            lax.all_gather(key_part, "inner", axis=0, tiled=True),
            lax.all_gather(value_part, "inner", axis=0, tiled=True),
        ),
        query_part,
        head_count,
    )
    gathered = lax.all_to_all(
        finish_state(running), "outer", split_axis=0, concat_axis=1, tiled=True
    )
    return gathered.reshape(unit_rows, networks, full_cols)


def attend_block(query, key, value):
    raw = lax.dot_general(
        query, key, (((1,), (1,)), ((), ())), preferred_element_type=jnp.float32
    )
    peak = jnp.max(raw, axis=1, keepdims=True)
    weights = jnp.exp2((raw - peak) * (math.log2(math.e) / math.sqrt(HEAD_DIM)))
    totals = jnp.sum(weights, axis=1, keepdims=True)
    numerator = jnp.dot(
        weights.astype(jnp.bfloat16), value, preferred_element_type=jnp.float32
    )
    return (numerator / totals).astype(jnp.bfloat16)


def exchange_kernel(
    outer, inner, heads,
    q_ref, k_ref, v_ref, out_ref,
    q_raw, k_raw, v_raw, k_buf, v_buf, o_raw,
    q_src, k_src, v_src, src_sem, local_sem, in_send, in_recv, out_send, out_recv,
):
    me_o, me_i = lax.axis_index("outer"), lax.axis_index("inner")
    tokens, networks, local_cols = q_ref.shape
    out_rows = out_ref.shape[0]
    half = outer // 2
    my_half, my_rest = me_o // half, me_o % half
    refs, raws = (k_src, v_src, q_src), (k_raw, v_raw, q_raw)

    def partner(step, sign):
        side = jnp.where(step < half, 1 - my_half, my_half)
        return side * half + (my_rest + sign * step + 2 * outer) % half

    def rows_of(block):
        return pl.ds(pl.multiple_of(block * tokens, tokens), tokens)

    def cols_of(head):
        return pl.ds(pl.multiple_of(head * HEAD_DIM, HEAD_DIM), HEAD_DIM)

    steps = [step for step in range(outer) if step != half]

    def in_copy(head, which, step, sign):
        other = partner(step, sign)
        target = other if sign == 1 else me_o
        source = me_o if sign == 1 else other
        return pltpu.make_async_remote_copy(
            src_ref=refs[which].at[:, :, cols_of(target * heads + head)],
            dst_ref=raws[which].at[head, rows_of(source)],
            send_sem=in_send,
            recv_sem=in_recv.at[head * 3 + which, step],
            device_id=(other, me_i),
            device_id_type=MESH,
        )

    def own_copy(head, which):
        return pltpu.make_async_copy(
            refs[which].at[:, :, cols_of(me_o * heads + head)],
            raws[which].at[head, rows_of(me_o)],
            local_sem.at[head * 3 + which],
        )

    def out_cols(source_o, source_i, head):
        return cols_of(source_i * (local_cols // HEAD_DIM) + source_o * heads + head)

    def out_slice(block, part):
        return pl.ds(block * tokens + part * out_rows, out_rows)

    def out_copy(head, block, part):
        return pltpu.make_async_remote_copy(
            src_ref=o_raw.at[head, out_slice(block, part)],
            dst_ref=out_ref.at[:, :, out_cols(me_o, me_i, head)],
            send_sem=out_send,
            recv_sem=out_recv,
            device_id=(block, part),
            device_id_type=MESH,
        )

    def out_own(head):
        return pltpu.make_async_copy(
            o_raw.at[head, out_slice(me_o, me_i)],
            out_ref.at[:, :, out_cols(me_o, me_i, head)],
            out_recv,
        )

    barrier = pltpu.get_barrier_semaphore()

    sources = [
        pltpu.make_async_copy(ref, kept, src_sem.at[which])
        for which, (ref, kept) in enumerate(zip((k_ref, v_ref, q_ref), refs))
    ]
    for copy in sources:
        copy.start()
    ends = [partner(step, 1) for step in steps]
    for shift in range(inner):
        part = (me_i + shift) % inner
        for other in ends:
            pl.semaphore_signal(barrier, inc=1, device_id=(other, part), device_id_type=MESH)
        if shift:
            pl.semaphore_signal(barrier, inc=1, device_id=(me_o, part), device_id_type=MESH)
    for copy in sources:
        copy.wait()
    pl.semaphore_wait(barrier, outer * inner - 1)

    for head in range(heads):
        for which in range(3):
            for step in steps:
                in_copy(head, which, step, 1).start()
            own_copy(head, which).start()

    both = networks * tokens
    split_row = lax.broadcasted_iota(jnp.int32, (both, both), 0)
    split_col = lax.broadcasted_iota(jnp.int32, (both, both), 1)
    split = (split_col == (split_row % tokens) * networks + split_row // tokens)
    split = split.astype(jnp.float32).astype(jnp.bfloat16)
    join = (split_row == (split_col % tokens) * networks + split_col // tokens)
    join = join.astype(jnp.float32).astype(jnp.bfloat16)

    def separate(raw, head, block):
        mixed = raw[head, rows_of(block)].reshape(both, HEAD_DIM)
        return jnp.dot(split, mixed, preferred_element_type=jnp.float32).astype(jnp.bfloat16)

    def place(head, which, block):
        apart = separate(raws[which], head, block)
        kept = (k_buf, v_buf)[which]
        for network in range(networks):
            kept[network, rows_of(block)] = apart[network * tokens:(network + 1) * tokens]

    def compute(head, block):
        query = separate(q_raw, head, block)
        parts = [
            attend_block(query[n * tokens:(n + 1) * tokens], k_buf[n], v_buf[n])
            for n in range(networks)
        ]
        mixed = jnp.dot(join, jnp.concatenate(parts, axis=0), preferred_element_type=jnp.float32)
        o_raw[head, rows_of(block)] = mixed.astype(jnp.bfloat16).reshape(
            tokens, networks, HEAD_DIM
        )

    for head in range(heads):
        for which in range(3):
            own_copy(head, which).wait()
        for which in range(2):
            place(head, which, me_o)

            def one_place(index, carry):
                step = jnp.where(index < half, index, index + 1)
                in_copy(head, which, step, -1).wait_recv()
                place(head, which, partner(step, -1))
                return carry

            lax.fori_loop(0, outer - 1, one_place, 0)

        compute(head, me_o)
        for shift in range(1, inner):
            out_copy(head, me_o, (me_i + shift) % inner).start()
        out_own(head).start()

        def one_block(index, carry):
            step = jnp.where(index < half, index, index + 1)
            in_copy(head, 2, step, -1).wait_recv()
            block = partner(step, -1)
            compute(head, block)
            for part in range(inner):
                out_copy(head, block, part).start()
            return carry

        lax.fori_loop(0, outer - 1, one_block, 0)

    def wait_bytes(ref, sem):
        pltpu.make_async_copy(ref, ref, sem).wait()

    for head in range(heads):
        for raw in raws:
            wait_bytes(raw.at[head, pl.ds(0, tokens * (outer - 1))], in_send)
        wait_bytes(o_raw.at[head, pl.ds(0, tokens * outer - out_rows)], out_send)
    wait_bytes(out_ref, out_recv)


def per_device(outer, inner, queries, keys, values):
    tokens, networks, local_cols = queries.shape
    heads = local_cols // HEAD_DIM // outer
    seq = tokens * outer
    out_rows = tokens // inner
    raw = pltpu.VMEM((heads, seq, networks, HEAD_DIM), jnp.bfloat16)
    kept = pltpu.VMEM((networks, seq, HEAD_DIM), jnp.bfloat16)
    return pl.pallas_call(
        partial(exchange_kernel, outer, inner, heads),
        out_shape=jax.ShapeDtypeStruct((out_rows, networks, local_cols * inner), jnp.bfloat16),
        in_specs=[pl.BlockSpec(memory_space=pl.ANY)] * 3,
        out_specs=pl.BlockSpec(memory_space=pl.ANY),
        scratch_shapes=[
            raw, raw, raw, kept, kept, raw,
            *[pltpu.VMEM(queries.shape, jnp.bfloat16)] * 3,
            pltpu.SemaphoreType.DMA((3,)),
            pltpu.SemaphoreType.DMA((heads * 3,)),
            pltpu.SemaphoreType.DMA,
            pltpu.SemaphoreType.DMA((heads * 3, outer)),
            pltpu.SemaphoreType.DMA,
            pltpu.SemaphoreType.DMA,
        ],
        compiler_params=pltpu.CompilerParams(collective_id=0, has_side_effects=True, vmem_limit_bytes=54500 * 1024),
    )(queries, keys, values)


def solution(mesh):
    outer, inner = mesh.shape["outer"], mesh.shape["inner"]

    def body(queries, keys, values):
        heads = queries.shape[2] // HEAD_DIM
        if outer % 2 == 0 and heads % outer == 0:
            return per_device(outer, inner, queries, keys, values)
        return per_device_split(queries, keys, values)

    return jax.shard_map(
        body,
        mesh=mesh,
        in_specs=(P("outer", None, "inner"),) * 3,
        out_specs=P(("outer", "inner"), None, None),
        check_vma=False,
    )
```
